256 devices in a mesh: ctx: 64 (over y_hi, z, x), tp: 4 (over y_lo, core).
Axes of the slice: x: 4, y: 4 (y_hi: 2, y_lo: 2; y = y_hi * 2 + y_lo), z: 8, core: 2. Of those that a mesh axis runs over, the one named last changes fastest.
Arguments:
- gate_branch: bfloat16 [4096, 16384], P('tp', 'ctx'), may hold values from -6 to 6
- key_branch: bfloat16 [4096, 16384], P('tp', 'ctx'), may hold values from -6 to 6
- value_branch: bfloat16 [4096, 16384], P('tp', 'ctx'), may hold values from -6 to 6
- long_filter: bfloat16 [4096, 16384], P('tp', 'ctx'), may hold values from -0.046875 to 0.046875
- skip_gain: float32 [4096], P('tp'), may hold values from 0.25 to 2
- out_weight: bfloat16 [4096, 4096], P(None, 'tp'), may hold values from -0.09375 to 0.09375
Outputs:
- mixer_out: bfloat16 [4096, 16384], P('tp', 'ctx')
The draws below stay inside these ranges and needn't reach their ends.
All inputs are finite; a program needn't handle non-finite values.
Results may differ from the reference program's by a relative error of at most 0.013.
Values may be sent and summed in bfloat16 or wider, within the bound.
A program may use at most 64 MiB of HBM per device.

```python
import math
import jax
import jax.numpy as jnp
from jax import lax

D = 4096
SEQ = 16384


def shard_levels(own_key, extent, shards, low, largest):
    level, own = 1.0, jax.random.fold_in(own_key, 6)
    for dim, blocks in shards:
        draws = jnp.exp(jax.random.uniform(jax.random.fold_in(own, dim), (blocks,), jnp.float32, low / len(shards), largest / len(shards)))
        level = level * jnp.repeat(draws, extent[dim] // blocks).reshape([-1 if axis == dim else 1 for axis in range(len(extent))])
    return level


def noise(stream_key, dims, spread, bound, shards=(), kind=jnp.bfloat16):
    entries = jax.random.normal(stream_key, dims, jnp.float32) * spread
    if len(shards) > 0:
        entries = shard_levels(stream_key, dims, shards, -0.22, 0.18) * entries
    return jnp.clip(entries, min=-bound, max=bound).astype(kind)


def setup_inputs(seed: int = 0) -> dict:
    key_list = jax.random.split(jax.random.key(seed), 7)
    return {
        "gate_branch": noise(key_list[0], (D, SEQ), 1.0, 6.0, ((0, 4), (1, 64))),
        "key_branch": noise(key_list[1], (D, SEQ), 1.0, 6.0, ((0, 4), (1, 64))),
        "value_branch": noise(key_list[2], (D, SEQ), 1.0, 6.0, ((0, 4), (1, 64))),
        "long_filter": noise(key_list[3], (D, SEQ), SEQ ** -0.5, 0.046875, ((0, 4), (1, 64))),
        "skip_gain": jnp.clip(jnp.exp(math.log(2.0) - 2.0794415 * jax.random.uniform(key_list[4], (D,), jnp.float32) ** shard_levels(key_list[4], (D,), ((0, 4),), -0.2, 0.2)), 0.25, 2.0),
        "out_weight": noise(key_list[5], (D, D), D ** -0.5, 0.09375, ((1, 4),)),
    }


def causal_block(pair):
    mixed_rows, filter_rows = pair
    length = 2 * SEQ
    left_spec = jnp.fft.rfft(mixed_rows.astype(jnp.float32), n=length, axis=-1)
    right_spec = jnp.fft.rfft(filter_rows.astype(jnp.float32), n=length, axis=-1)
    result = jnp.fft.irfft(left_spec * right_spec, n=length, axis=-1)[:, :SEQ]
    return result.astype(jnp.bfloat16)


def reference(gate_branch, key_branch, value_branch, long_filter, skip_gain, out_weight):
    mixed = (key_branch.astype(jnp.float32) * value_branch.astype(jnp.float32)).astype(jnp.bfloat16)
    blocks = D // 128
    conv = lax.map(causal_block, (mixed.reshape(blocks, 128, SEQ), long_filter.reshape(blocks, 128, SEQ)))
    conv = conv.reshape(D, SEQ)
    gated = gate_branch.astype(jnp.float32) * (conv.astype(jnp.float32) + skip_gain[:, None] * mixed.astype(jnp.float32))
    gated = gated.astype(jnp.bfloat16)
    output = jnp.dot(out_weight.astype(jnp.float32), gated.astype(jnp.float32), preferred_element_type=jnp.float32)
    return output.astype(jnp.bfloat16)
```

```python
import functools

import jax
import jax.numpy as jnp
import numpy as np
from jax import lax
from jax.experimental import pallas as pl
from jax.experimental.pallas import tpu as pltpu
from jax.sharding import PartitionSpec as P

MESH = pl.DeviceIdType.MESH
CTX = 64
TP = 4
BASE = 128
CHUNKS = 2
GROUP = 8


def tables():
    index = np.arange(BASE)
    first = np.exp(2j * np.pi * np.outer(index + 0.25, index) / BASE)
    twist = np.exp(2j * np.pi * np.outer(index + 0.25, index) / BASE**2)
    second = np.exp(2j * np.pi * np.outer(index, index) / BASE)
    back = first.T / BASE**2
    low = lambda table: jnp.asarray(table, jnp.bfloat16)
    return (
        low(np.concatenate([first.real, first.imag], 0)),
        low(np.block([[second.real, second.imag], [-second.imag, second.real]])),
        low(np.block([[second.real, -second.imag], [second.imag, second.real]])),
        low(np.concatenate([back.real, back.imag], 1)),
        jnp.asarray(np.stack([twist.real, twist.imag]), jnp.float32),
    )


def peer(me, offset):
    high, z, x = me // 32, (me // 4) % 8, me % 4
    return (
        ((high + offset // 32) % 2) * 32
        + ((z + (offset // 4) % 8) % 8) * 4
        + (x + offset % 4) % 4
    )


def dot(left, right):
    return jnp.dot(left, right, preferred_element_type=jnp.float32)


def kernel(
    gate_hbm,
    key_hbm,
    value_hbm,
    filter_hbm,
    skip_ref,
    weight_hbm,
    first_ref,
    second_ref,
    second_back_ref,
    first_back_ref,
    twist_ref,
    out_ref,
    gate,
    key,
    value,
    taps,
    weight,
    mixed,
    skipped,
    in_mixed,
    in_taps,
    stage_mixed,
    stage_taps,
    stage_out,
    back_send,
    back_recv,
    gated,
    core_send,
    core_recv,
    keep,
    y_send,
    y_recv,
    load_sem,
    in_send_sem,
    in_recv_sem,
    back_send_sem,
    back_recv_sem,
    core_send_sem,
    core_recv_sem,
    y_send_sem,
    y_recv_sem,
):
    me, tp = lax.axis_index("ctx"), lax.axis_index("tp")
    side, core = tp // 2, tp % 2
    mate = side * 2 + 1 - core
    across = (1 - side) * 2 + core

    barrier = pltpu.get_barrier_semaphore()

    def greet(offset, carry):
        pl.semaphore_signal(
            barrier, inc=1, device_id={"ctx": peer(me, offset)}, device_id_type=MESH
        )
        return carry

    lax.fori_loop(1, CTX, greet, 0)
    for other in (mate, across):
        pl.semaphore_signal(barrier, inc=1, device_id={"tp": other}, device_id_type=MESH)

    loads = [
        pltpu.make_async_copy(source, target, load_sem.at[slot])
        for slot, (source, target) in enumerate(
            (
                (key_hbm, key),
                (value_hbm, value),
                (filter_hbm, taps),
                (gate_hbm, gate),
                (weight_hbm, weight),
            )
        )
    ]
    for load in loads:
        load.start()
    loads[0].wait()
    loads[1].wait()

    def multiply(row, carry):
        product = key[row].astype(jnp.float32) * value[row].astype(jnp.float32)
        mixed[row] = product.astype(jnp.bfloat16)
        return carry

    lax.fori_loop(0, CTX, multiply, 0, unroll=4)
    for part in range(8):
        spread = jnp.broadcast_to(skip_ref[part : part + 1, :], (128, 128)).T
        for half in range(2):
            rows = mixed[part * 8 : part * 8 + 8, :, :, half * 128 : half * 128 + 128]
            rows = rows.astype(jnp.float32).reshape(128, 128)
            skipped[half, part * 128 : part * 128 + 128, :] = spread * rows
    loads[2].wait()

    pl.semaphore_wait(barrier, CTX + 1)

    def sent_in(chunk, which, target):
        source, landing = ((taps, in_taps), (mixed, in_mixed))[which]
        return pltpu.make_async_remote_copy(
            src_ref=source.at[target, chunk],
            dst_ref=landing.at[chunk, me],
            send_sem=in_send_sem.at[chunk, which],
            recv_sem=in_recv_sem.at[chunk, which],
            device_id={"ctx": target},
            device_id_type=MESH,
        )

    for chunk in range(CHUNKS):

        def push(offset, carry, chunk=chunk):
            target = peer(me, offset)
            sent_in(chunk, 0, target).start()
            sent_in(chunk, 1, target).start()
            return carry

        lax.fori_loop(1, CTX, push, 0)
    for chunk in range(CHUNKS):
        in_taps[chunk, me] = taps[me, chunk]
        in_mixed[chunk, me] = mixed[me, chunk]

    def wait_in(chunk, which, receive):
        source, landing = ((taps, in_taps), (mixed, in_mixed))[which]
        whole = landing.at[chunk, pl.ds(0, CTX - 1)]
        copy = pltpu.make_async_remote_copy(
            src_ref=whole,
            dst_ref=whole,
            send_sem=in_send_sem.at[chunk, which],
            recv_sem=in_recv_sem.at[chunk, which],
            device_id={"ctx": peer(me, 1)},
            device_id_type=MESH,
        )
        if receive:
            copy.wait_recv()
        else:
            copy.wait_send()

    def transform(stage, channel):
        rows = stage.reshape(BASE * GROUP, BASE)[pl.ds(channel, BASE, stride=GROUP), :]
        both = dot(first_ref[...], rows.astype(jnp.bfloat16))
        real, imag = both[:BASE], both[BASE:]
        cos, sin = twist_ref[0], twist_ref[1]
        turned = jnp.concatenate([real * cos - imag * sin, real * sin + imag * cos], 1)
        return dot(turned.astype(jnp.bfloat16), second_ref[...])

    for chunk in range(CHUNKS):
        wait_in(chunk, 0, True)
        wait_in(chunk, 1, True)

        def spread(row, carry, chunk=chunk):
            for landing, stage in ((in_taps, stage_taps), (in_mixed, stage_mixed)):
                block = landing[chunk, row].astype(jnp.float32)
                stage[row, 0] = block[:, :128]
                stage[row, 1] = block[:, 128:]
            return carry

        lax.fori_loop(0, CTX, spread, 0, unroll=8)

        for channel in range(GROUP):
            left = transform(stage_taps, channel)
            right = transform(stage_mixed, channel)
            left_real, left_imag = left[:, :BASE], left[:, BASE:]
            right_real, right_imag = right[:, :BASE], right[:, BASE:]
            product = jnp.concatenate(
                [
                    left_real * right_real - left_imag * right_imag,
                    left_real * right_imag + left_imag * right_real,
                ],
                1,
            )
            back = dot(product.astype(jnp.bfloat16), second_back_ref[...])
            real, imag = back[:, :BASE], back[:, BASE:]
            cos, sin = twist_ref[0], twist_ref[1]
            unturned = jnp.concatenate([real * cos + imag * sin, imag * cos - real * sin], 0)
            conv = dot(first_back_ref[...], unturned.astype(jnp.bfloat16))
            stage_out.reshape(BASE * GROUP, BASE)[pl.ds(channel, BASE, stride=GROUP), :] = conv

        def gather(row, carry, chunk=chunk):
            for half in range(2):
                back_send[half, chunk, row] = stage_out[row, half].astype(jnp.bfloat16)
            return carry

        lax.fori_loop(0, CTX, gather, 0, unroll=8)
        for half in range(2):

            def push_back(offset, carry, half=half, chunk=chunk):
                target = peer(me, offset)
                pltpu.make_async_remote_copy(
                    src_ref=back_send.at[half, chunk, target],
                    dst_ref=back_recv.at[half, me * CHUNKS + chunk],
                    send_sem=back_send_sem.at[half],
                    recv_sem=back_recv_sem.at[half],
                    device_id={"ctx": target},
                    device_id_type=MESH,
                ).start()
                return carry

            lax.fori_loop(1, CTX, push_back, 0)
            back_recv[half, me * CHUNKS + chunk] = back_send[half, chunk, me]

    def wait_back(half):
        whole = back_recv.at[half, pl.ds(0, (CTX - 1) * CHUNKS)]
        return pltpu.make_async_remote_copy(
            src_ref=whole,
            dst_ref=whole,
            send_sem=back_send_sem.at[half],
            recv_sem=back_recv_sem.at[half],
            device_id={"ctx": peer(me, 1)},
            device_id_type=MESH,
        )

    def to_mate(half, slot):
        return pltpu.make_async_remote_copy(
            src_ref=core_send.at[half, slot],
            dst_ref=core_recv.at[half, slot],
            send_sem=core_send_sem.at[half, slot],
            recv_sem=core_recv_sem.at[half, slot],
            device_id={"tp": mate},
            device_id_type=MESH,
        )

    def to_across(half):
        return pltpu.make_async_remote_copy(
            src_ref=y_send.at[half],
            dst_ref=y_recv.at[half],
            send_sem=y_send_sem.at[half],
            recv_sem=y_recv_sem.at[half],
            device_id={"tp": across},
            device_id_type=MESH,
        )

    tile = 256

    def project(half, block, store):
        def step(index, carry):
            start = pl.multiple_of(index * tile, tile)
            rows = weight[pl.ds(pl.multiple_of(block * 1024, 1024) + start, tile), :]
            store(pl.ds(start, tile), dot(rows, gated[half]))
            return carry

        lax.fori_loop(0, 1024 // tile, step, 0)

    loads[3].wait()
    loads[4].wait()
    for half in range(2):
        wait_back(half).wait_recv()
        for part in range(8):
            lanes = slice(half * 128, half * 128 + 128)
            block = slice(part * 16, part * 16 + 16)
            conv = back_recv[half, block].astype(jnp.float32).reshape(128, 128)
            gates = gate[block, :, lanes].astype(jnp.float32).reshape(128, 128)
            rows = slice(part * 128, part * 128 + 128)
            gated[half, rows, :] = (gates * (conv + skipped[half, rows, :])).astype(jnp.bfloat16)

        for slot, owner in enumerate((1 - side, side)):

            def send_rows(rows, value, half=half, slot=slot):
                core_send[half, slot, rows, :] = value.astype(jnp.bfloat16)

            def keep_rows(rows, value, half=half, slot=slot):
                keep[half, slot, rows, :] = value

            project(half, owner * 2 + 1 - core, send_rows)
            to_mate(half, slot).start()
            project(half, owner * 2 + core, keep_rows)
            to_mate(half, slot).wait_recv()
            if slot == 0:
                summed = keep[half, 0] + core_recv[half, 0].astype(jnp.float32)
                y_send[half] = summed.astype(jnp.bfloat16)
                to_across(half).start()

    for half in range(2):
        to_across(half).wait_recv()
        total = (
            keep[half, 1]
            + core_recv[half, 1].astype(jnp.float32)
            + y_recv[half].astype(jnp.float32)
        )
        out_ref[:, half * 128 : half * 128 + 128] = total.astype(jnp.bfloat16)

    for chunk in range(CHUNKS):
        wait_in(chunk, 0, False)
        wait_in(chunk, 1, False)
    for half in range(2):
        wait_back(half).wait_send()
        to_mate(half, 0).wait_send()
        to_mate(half, 1).wait_send()
        to_across(half).wait_send()


def body(gate_branch, key_branch, value_branch, long_filter, skip_gain, out_weight):
    low, full = jnp.bfloat16, jnp.float32
    dma = pltpu.SemaphoreType.DMA
    messages = (CTX, CHUNKS, GROUP, 256)
    anywhere = pl.BlockSpec(memory_space=pl.ANY)
    local = pl.BlockSpec(memory_space=pltpu.VMEM)
    return pl.pallas_call(
        kernel,
        out_shape=jax.ShapeDtypeStruct((1024, 256), low),
        in_specs=[anywhere] * 4 + [local] + [anywhere] + [local] * 5,
        out_specs=local,
        scratch_shapes=[
            pltpu.VMEM((128, 8, 256), low),
            pltpu.VMEM(messages, low),
            pltpu.VMEM(messages, low),
            pltpu.VMEM(messages, low),
            pltpu.VMEM((4096, 1024), low),
            pltpu.VMEM(messages, low),
            pltpu.VMEM((2, 1024, 128), full),
            pltpu.VMEM((CHUNKS, CTX, GROUP, 256), low),
            pltpu.VMEM((CHUNKS, CTX, GROUP, 256), low),
            pltpu.VMEM((CTX, 2, GROUP, 128), full),
            pltpu.VMEM((CTX, 2, GROUP, 128), full),
            pltpu.VMEM((CTX, 2, GROUP, 128), full),
            pltpu.VMEM((2, CHUNKS, CTX, GROUP, 128), low),
            pltpu.VMEM((2, CTX * CHUNKS, GROUP, 128), low),
            pltpu.VMEM((2, 1024, 128), low),
            pltpu.VMEM((2, 2, 1024, 128), low),
            pltpu.VMEM((2, 2, 1024, 128), low),
            pltpu.VMEM((2, 2, 1024, 128), full),
            pltpu.VMEM((2, 1024, 128), low),
            pltpu.VMEM((2, 1024, 128), low),
            dma((5,)),
            dma((CHUNKS, 2)),
            dma((CHUNKS, 2)),
            dma((2,)),
            dma((2,)),
            dma((2, 2)),
            dma((2, 2)),
            dma((2,)),
            dma((2,)),
        ],
        compiler_params=pltpu.CompilerParams(
            collective_id=0, has_side_effects=True, vmem_limit_bytes=60 * 1024 * 1024
        ),
    )(
        gate_branch.reshape(128, 8, 256),
        key_branch.reshape(messages),
        value_branch.reshape(messages),
        long_filter.reshape(messages),
        skip_gain.reshape(8, 128),
        out_weight,
        *tables(),
    )


def solution(mesh):
    placed = (
        P("tp", "ctx"),
        P("tp", "ctx"),
        P("tp", "ctx"),
        P("tp", "ctx"),
        P("tp"),
        P(None, "tp"),
    )
    return jax.shard_map(
        body, mesh=mesh, in_specs=placed, out_specs=P("tp", "ctx"), check_vma=False
    )
```

```python
import functools

import jax
import jax.numpy as jnp
import numpy as np
from jax import lax
from jax.experimental import pallas as pl
from jax.experimental.pallas import tpu as pltpu
from jax.sharding import PartitionSpec as P

MESH = pl.DeviceIdType.MESH
CTX = 64
TP = 4
BASE = 128
CHUNKS = 2
GROUP = 8
PIECE = 256
PIECES = 1024 // PIECE


def tables():
    index = np.arange(BASE)
    first = np.exp(2j * np.pi * np.outer(index + 0.25, index) / BASE)
    twist = np.exp(2j * np.pi * np.outer(index + 0.25, index) / BASE**2)
    second = np.exp(2j * np.pi * np.outer(index, index) / BASE)
    back = first.T / BASE**2
    low = lambda table: jnp.asarray(table, jnp.bfloat16)
    return (
        low(np.concatenate([first.real, first.imag], 0)),
        low(np.block([[second.real, second.imag], [-second.imag, second.real]])),
        low(np.block([[second.real, -second.imag], [second.imag, second.real]])),
        low(np.concatenate([back.real, back.imag], 1)),
        jnp.asarray(np.stack([twist.real, twist.imag]), jnp.float32),
    )


def every_peer(me, act):
    high, z, x = me // 32 * 32, (me // 4) % 8, me % 4
    near = [(x + step) % 4 for step in range(4)]
    far = [(z + step) % 8 * 4 for step in range(8)]
    halves = (high, 32 - high)
    for dz, dy, dx in ORDER:
        act(halves[dy] + far[dz] + near[dx])


ORDER = [(4, 1, 2), (3, 1, 2), (4, 1, 1), (4, 1, 3), (5, 1, 2), (2, 1, 2), (3, 1, 1), (3, 1, 3), (4, 0, 2), (4, 1, 0), (5, 1, 1), (5, 1, 3), (6, 1, 2), (1, 1, 2), (2, 1, 1), (2, 1, 3), (3, 0, 2), (3, 1, 0), (4, 0, 1), (4, 0, 3), (5, 0, 2), (5, 1, 0), (6, 1, 1), (6, 1, 3), (7, 1, 2), (0, 1, 2), (1, 1, 1), (1, 1, 3), (2, 0, 2), (2, 1, 0), (3, 0, 1), (3, 0, 3), (4, 0, 0), (5, 0, 1), (5, 0, 3), (6, 0, 2), (6, 1, 0), (7, 1, 1), (7, 1, 3), (0, 1, 1), (0, 1, 3), (1, 0, 2), (1, 1, 0), (2, 0, 1), (2, 0, 3), (3, 0, 0), (5, 0, 0), (6, 0, 1), (6, 0, 3), (7, 0, 2), (7, 1, 0), (0, 0, 2), (0, 1, 0), (1, 0, 1), (1, 0, 3), (2, 0, 0), (6, 0, 0), (7, 0, 1), (7, 0, 3), (0, 0, 1), (0, 0, 3), (1, 0, 0), (7, 0, 0)]


def dot(left, right):
    return jnp.dot(left, right, preferred_element_type=jnp.float32)


def kernel(
    gate_hbm,
    key_hbm,
    value_hbm,
    filter_hbm,
    skip_ref,
    weight_hbm,
    first_ref,
    second_ref,
    second_back_ref,
    first_back_ref,
    twist_ref,
    own_hbm,
    other_hbm,
    gate,
    key,
    value,
    taps,
    weight,
    mixed,
    skipped,
    in_mixed,
    in_taps,
    stage_mixed,
    stage_taps,
    stage_out,
    spectra_taps,
    back_send,
    back_recv,
    gated,
    core_send,
    core_recv,
    keep,
    y_send,
    own,
    load_sem,
    in_send_sem,
    in_recv_sem,
    back_send_sem,
    back_recv_sem,
    core_send_sem,
    core_recv_sem,
    y_send_sem,
    y_recv_sem,
    own_sem,
):
    me, tp = lax.axis_index("ctx"), lax.axis_index("tp")
    side, core = tp // 2, tp % 2
    mate = side * 2 + 1 - core
    across = (1 - side) * 2 + core

    barrier = pltpu.get_barrier_semaphore()

    loads = [
        pltpu.make_async_copy(source, target, load_sem.at[slot])
        for slot, (source, target) in enumerate(
            (
                (filter_hbm, taps),
                (key_hbm, key),
                (value_hbm, value),
                (gate_hbm, gate),
                (weight_hbm, weight),
            )
        )
    ]
    loads[0].start()
    every_peer(
        me,
        lambda other: pl.semaphore_signal(
            barrier, inc=1, device_id={"ctx": other}, device_id_type=MESH
        ),
    )
    for other in (mate, across):
        pl.semaphore_signal(barrier, inc=1, device_id={"tp": other}, device_id_type=MESH)

    for load in loads[1:]:
        load.start()

    def multiply(chunk):
        def step(row, carry):
            product = key[row, chunk].astype(jnp.float32) * value[row, chunk].astype(jnp.float32)
            mixed[row, chunk] = product.astype(jnp.bfloat16)
            return carry

        lax.fori_loop(0, CTX, step, 0, unroll=8)

    def skip():
        for part in range(8):
            spread = jnp.broadcast_to(skip_ref[part : part + 1, :], (128, 128)).T
            for half in range(2):
                rows = mixed[part * 8 : part * 8 + 8, :, :, half * 128 : half * 128 + 128]
                rows = rows.astype(jnp.float32).reshape(128, 128)
                skipped[half, part * 128 : part * 128 + 128, :] = spread * rows

    def sent_in(chunk, which, target):
        source, landing = ((taps, in_taps), (mixed, in_mixed))[which]
        return pltpu.make_async_remote_copy(
            src_ref=source.at[target, chunk],
            dst_ref=landing.at[chunk, me],
            send_sem=in_send_sem.at[chunk, which],
            recv_sem=in_recv_sem.at[chunk, which],
            device_id={"ctx": target},
            device_id_type=MESH,
        )

    def push_in(chunk, which):
        every_peer(me, lambda other: sent_in(chunk, which, other).start())
        source, landing = ((taps, in_taps), (mixed, in_mixed))[which]
        landing[chunk, me] = source[me, chunk]

    def wait_in(chunk, which, receive):
        source, landing = ((taps, in_taps), (mixed, in_mixed))[which]
        whole = landing.at[chunk, pl.ds(0, CTX - 1)]
        copy = pltpu.make_async_remote_copy(
            src_ref=whole,
            dst_ref=whole,
            send_sem=in_send_sem.at[chunk, which],
            recv_sem=in_recv_sem.at[chunk, which],
            device_id={"ctx": (me + 1) % CTX},
            device_id_type=MESH,
        )
        if receive:
            copy.wait_recv()
        else:
            copy.wait_send()

    cos, sin = twist_ref[0], twist_ref[1]

    def spread(chunk, landing, stage):
        def step(row, carry):
            block = landing[chunk, row].astype(jnp.float32)
            stage[row, 0] = block[:, :128]
            stage[row, 1] = block[:, 128:]
            return carry

        lax.fori_loop(0, CTX, step, 0, unroll=8)

    def transform(stage, pair):
        flat = stage.reshape(BASE * GROUP, BASE)
        rows = [flat[pl.ds(2 * pair + one, BASE, stride=GROUP), :] for one in range(2)]
        both = dot(first_ref[...], jnp.concatenate(rows, 1).astype(jnp.bfloat16))
        spectra = []
        for one in range(2):
            real = both[:BASE, one * BASE : one * BASE + BASE]
            imag = both[BASE:, one * BASE : one * BASE + BASE]
            turned = jnp.concatenate([real * cos - imag * sin, real * sin + imag * cos], 1)
            spectra.append(dot(turned.astype(jnp.bfloat16), second_ref[...]))
        return spectra

    def transform_taps(chunk):
        spread(chunk, in_taps, stage_taps)
        for pair in range(GROUP // 2):
            for one, spectrum in enumerate(transform(stage_taps, pair)):
                spectra_taps[chunk, 2 * pair + one] = spectrum

    def convolve(chunk):
        spread(chunk, in_mixed, stage_mixed)
        for pair in range(GROUP // 2):
            halves = []
            for one, right in enumerate(transform(stage_mixed, pair)):
                left = spectra_taps[chunk, 2 * pair + one]
                left_real, left_imag = left[:, :BASE], left[:, BASE:]
                right_real, right_imag = right[:, :BASE], right[:, BASE:]
                product = jnp.concatenate(
                    [
                        left_real * right_real - left_imag * right_imag,
                        left_real * right_imag + left_imag * right_real,
                    ],
                    1,
                )
                back = dot(product.astype(jnp.bfloat16), second_back_ref[...])
                real, imag = back[:, :BASE], back[:, BASE:]
                halves.append(
                    jnp.concatenate([real * cos + imag * sin, imag * cos - real * sin], 0)
                )
            unturned = jnp.concatenate(halves, 1).astype(jnp.bfloat16)
            conv = dot(first_back_ref[...], unturned)
            flat = stage_out.reshape(BASE * GROUP, BASE)
            for one in range(2):
                flat[pl.ds(2 * pair + one, BASE, stride=GROUP), :] = conv[
                    :, one * BASE : one * BASE + BASE
                ]

        def gather(row, carry):
            for half in range(2):
                back_send[half, chunk, row] = stage_out[row, half].astype(jnp.bfloat16)
            return carry

        lax.fori_loop(0, CTX, gather, 0, unroll=8)
        for half in range(2):
            back_recv[half, me * CHUNKS + chunk] = back_send[half, chunk, me]

    def push_back(half, chunk):
        def send(target):
            pltpu.make_async_remote_copy(
                src_ref=back_send.at[half, chunk, target],
                dst_ref=back_recv.at[half, me * CHUNKS + chunk],
                send_sem=back_send_sem.at[half],
                recv_sem=back_recv_sem.at[half],
                device_id={"ctx": target},
                device_id_type=MESH,
            ).start()

        every_peer(me, send)

    loads[0].wait()
    pl.semaphore_wait(barrier, CTX + 1)
    push_in(0, 0)
    push_in(1, 0)
    loads[1].wait()
    loads[2].wait()
    multiply(0)
    push_in(0, 1)
    multiply(1)
    push_in(1, 1)
    skip()
    wait_in(0, 0, True)
    transform_taps(0)
    wait_in(1, 0, True)
    transform_taps(1)
    wait_in(0, 1, True)
    convolve(0)
    push_back(0, 0)
    wait_in(1, 1, True)
    convolve(1)
    push_back(0, 1)
    push_back(1, 0)
    push_back(1, 1)

    def wait_back(half):
        whole = back_recv.at[half, pl.ds(0, (CTX - 1) * CHUNKS)]
        return pltpu.make_async_remote_copy(
            src_ref=whole,
            dst_ref=whole,
            send_sem=back_send_sem.at[half],
            recv_sem=back_recv_sem.at[half],
            device_id={"ctx": (me + 1) % CTX},
            device_id_type=MESH,
        )

    def to_mate(half, slot, piece):
        rows = pl.ds(pl.multiple_of(piece * PIECE, PIECE), PIECE)
        return pltpu.make_async_remote_copy(
            src_ref=core_send.at[half, slot, rows],
            dst_ref=core_recv.at[half, slot, rows],
            send_sem=core_send_sem.at[half, slot, piece],
            recv_sem=core_recv_sem.at[half, slot, piece],
            device_id={"tp": mate},
            device_id_type=MESH,
        )

    def to_across(half, rows):
        return pltpu.make_async_remote_copy(
            src_ref=y_send.at[half, rows],
            dst_ref=other_hbm.at[rows, pl.ds(half * 128, 128)],
            send_sem=y_send_sem.at[half],
            recv_sem=y_recv_sem.at[half],
            device_id={"tp": across},
            device_id_type=MESH,
        )

    def own_out(half):
        return pltpu.make_async_copy(
            own.at[half], own_hbm.at[:, pl.ds(half * 128, 128)], own_sem.at[half]
        )

    loads[3].wait()
    loads[4].wait()
    for half in range(2):
        wait_back(half).wait_recv()
        for part in range(8):
            lanes = slice(half * 128, half * 128 + 128)
            block = slice(part * 16, part * 16 + 16)
            conv = back_recv[half, block].astype(jnp.float32).reshape(128, 128)
            gates = gate[block, :, lanes].astype(jnp.float32).reshape(128, 128)
            rows = slice(part * 128, part * 128 + 128)
            gated[half, rows, :] = (gates * (conv + skipped[half, rows, :])).astype(jnp.bfloat16)

        def project(step, half=half):
            slot, piece = step // PIECES, step % PIECES
            owner = (side + 1 - slot) % 2
            rows = pl.ds(pl.multiple_of(piece * PIECE, PIECE), PIECE)

            def part(block):
                start = pl.multiple_of(block * 1024 + piece * PIECE, PIECE)
                return dot(weight[pl.ds(start, PIECE), :], gated[half])

            core_send[half, slot, rows, :] = part(owner * 2 + 1 - core).astype(jnp.bfloat16)
            to_mate(half, slot, piece).start()
            keep[half, slot, rows, :] = part(owner * 2 + core)

        def combine(step, half=half):
            slot, piece = step // PIECES, step % PIECES
            rows = pl.ds(pl.multiple_of(piece * PIECE, PIECE), PIECE)
            to_mate(half, slot, piece).wait_recv()
            summed = keep[half, slot, rows, :] + core_recv[half, slot, rows, :].astype(jnp.float32)

            @pl.when(slot == 0)
            def _():
                y_send[half, rows, :] = summed.astype(jnp.bfloat16)
                to_across(half, rows).start()

            @pl.when(slot == 1)
            def _():
                own[half, rows, :] = summed.astype(jnp.bfloat16)

        def advance(step, carry):
            project(step)

            @pl.when(step > 0)
            def _():
                combine(step - 1)

            return carry

        lax.fori_loop(0, 2 * PIECES, advance, 0)
        combine(2 * PIECES - 1)
        own_out(half).start()

    for chunk in range(CHUNKS):
        wait_in(chunk, 0, False)
        wait_in(chunk, 1, False)
    for half in range(2):
        wait_back(half).wait_send()
        for slot in range(2):
            for piece in range(PIECES):
                to_mate(half, slot, piece).wait_send()
        own_out(half).wait()
        to_across(half, pl.ds(0, 1024)).wait_send()
        to_across(half, pl.ds(0, 1024)).wait_recv()


def body(gate_branch, key_branch, value_branch, long_filter, skip_gain, out_weight):
    low, full = jnp.bfloat16, jnp.float32
    dma = pltpu.SemaphoreType.DMA
    messages = (CTX, CHUNKS, GROUP, 256)
    anywhere = pl.BlockSpec(memory_space=pl.ANY)
    local = pl.BlockSpec(memory_space=pltpu.VMEM)
    own, other = pl.pallas_call(
        kernel,
        out_shape=[jax.ShapeDtypeStruct((1024, 256), low)] * 2,
        in_specs=[anywhere] * 4 + [local] + [anywhere] + [local] * 5,
        out_specs=[anywhere] * 2,
        scratch_shapes=[
            pltpu.VMEM((128, 8, 256), low),
            pltpu.VMEM(messages, low),
            pltpu.VMEM(messages, low),
            pltpu.VMEM(messages, low),
            pltpu.VMEM((4096, 1024), low),
            pltpu.VMEM(messages, low),
            pltpu.VMEM((2, 1024, 128), full),
            pltpu.VMEM((CHUNKS, CTX, GROUP, 256), low),
            pltpu.VMEM((CHUNKS, CTX, GROUP, 256), low),
            pltpu.VMEM((CTX, 2, GROUP, 128), full),
            pltpu.VMEM((CTX, 2, GROUP, 128), full),
            pltpu.VMEM((CTX, 2, GROUP, 128), full),
            pltpu.VMEM((CHUNKS, GROUP, BASE, 2 * BASE), full),
            pltpu.VMEM((2, CHUNKS, CTX, GROUP, 128), low),
            pltpu.VMEM((2, CTX * CHUNKS, GROUP, 128), low),
            pltpu.VMEM((2, 1024, 128), low),
            pltpu.VMEM((2, 2, 1024, 128), low),
            pltpu.VMEM((2, 2, 1024, 128), low),
            pltpu.VMEM((2, 2, 1024, 128), full),
            pltpu.VMEM((2, 1024, 128), low),
            pltpu.VMEM((2, 1024, 128), low),
            dma((5,)),
            dma((CHUNKS, 2)),
            dma((CHUNKS, 2)),
            dma((2,)),
            dma((2,)),
            dma((2, 2, PIECES)),
            dma((2, 2, PIECES)),
            dma((2,)),
            dma((2,)),
            dma((2,)),
        ],
        compiler_params=pltpu.CompilerParams(
            collective_id=0, has_side_effects=True, vmem_limit_bytes=60 * 1024 * 1024
        ),
    )(
        gate_branch.reshape(128, 8, 256),
        key_branch.reshape(messages),
        value_branch.reshape(messages),
        long_filter.reshape(messages),
        skip_gain.reshape(8, 128),
        out_weight,
        *tables(),
    )
    return (own.astype(full) + other.astype(full)).astype(low)


def solution(mesh):
    placed = (
        P("tp", "ctx"),
        P("tp", "ctx"),
        P("tp", "ctx"),
        P("tp", "ctx"),
        P("tp"),
        P(None, "tp"),
    )
    return jax.shard_map(
        body, mesh=mesh, in_specs=placed, out_specs=P("tp", "ctx"), check_vma=False
    )
```

```python
import functools

import jax
import jax.numpy as jnp
import numpy as np
from jax import lax
from jax.experimental import pallas as pl
from jax.experimental.pallas import tpu as pltpu
from jax.sharding import PartitionSpec as P

MESH = pl.DeviceIdType.MESH
CTX = 64
TP = 4
BASE = 128
CHUNKS = 2
GROUP = 8
SPAN = 8
PIECE = 256
PIECES = 1024 // PIECE


def tables():
    index = np.arange(BASE)
    first = np.exp(2j * np.pi * np.outer(index + 0.25, index) / BASE)
    twist = np.exp(2j * np.pi * np.outer(index + 0.25, index) / BASE**2)
    second = np.exp(2j * np.pi * np.outer(index, index) / BASE)
    back = first.T / BASE**2
    low = lambda table: jnp.asarray(table, jnp.bfloat16)
    return (
        low(np.concatenate([first.real, first.imag], 0)),
        low(np.block([[second.real, second.imag], [-second.imag, second.real]])),
        low(np.block([[second.real, -second.imag], [second.imag, second.real]])),
        low(np.concatenate([back.real, back.imag], 1)),
        jnp.asarray(np.stack([twist.real, twist.imag]), jnp.float32),
    )


def every_peer(me, act):
    high, z, x = me // 32 * 32, (me // 4) % 8, me % 4
    near = [(x + step) % 4 for step in range(4)]
    far = [(z + step) % 8 * 4 for step in range(8)]
    halves = (high, 32 - high)
    for dz, dy, dx in ORDER:
        act(halves[dy] + far[dz] + near[dx])


ORDER = [(4, 1, 2), (3, 1, 2), (4, 1, 1), (4, 1, 3), (5, 1, 2), (2, 1, 2), (3, 1, 1), (3, 1, 3), (4, 0, 2), (4, 1, 0), (5, 1, 1), (5, 1, 3), (6, 1, 2), (1, 1, 2), (2, 1, 1), (2, 1, 3), (3, 0, 2), (3, 1, 0), (4, 0, 1), (4, 0, 3), (5, 0, 2), (5, 1, 0), (6, 1, 1), (6, 1, 3), (7, 1, 2), (0, 1, 2), (1, 1, 1), (1, 1, 3), (2, 0, 2), (2, 1, 0), (3, 0, 1), (3, 0, 3), (4, 0, 0), (5, 0, 1), (5, 0, 3), (6, 0, 2), (6, 1, 0), (7, 1, 1), (7, 1, 3), (0, 1, 1), (0, 1, 3), (1, 0, 2), (1, 1, 0), (2, 0, 1), (2, 0, 3), (3, 0, 0), (5, 0, 0), (6, 0, 1), (6, 0, 3), (7, 0, 2), (7, 1, 0), (0, 0, 2), (0, 1, 0), (1, 0, 1), (1, 0, 3), (2, 0, 0), (6, 0, 0), (7, 0, 1), (7, 0, 3), (0, 0, 1), (0, 0, 3), (1, 0, 0), (7, 0, 0)]


def dot(left, right):
    return jnp.dot(left, right, preferred_element_type=jnp.float32)


def kernel(
    gate_hbm,
    key_hbm,
    value_hbm,
    filter_hbm,
    skip_hbm,
    weight_hbm,
    first_hbm,
    second_hbm,
    second_back_hbm,
    first_back_hbm,
    twist_hbm,
    own_hbm,
    other_hbm,
    gate,
    key,
    value,
    taps,
    weight,
    mixed,
    skipped,
    in_mixed,
    in_taps,
    stage_mixed,
    stage_taps,
    stage_out,
    spectra_taps,
    back_send,
    back_recv,
    gated,
    core_send,
    core_recv,
    keep,
    y_send,
    own,
    skip_ref,
    first_ref,
    second_ref,
    second_back_ref,
    first_back_ref,
    twist_ref,
    load_sem,
    in_send_sem,
    in_recv_sem,
    back_send_sem,
    back_recv_sem,
    core_send_sem,
    core_recv_sem,
    y_send_sem,
    y_recv_sem,
    own_sem,
):
    me, tp = lax.axis_index("ctx"), lax.axis_index("tp")
    side, core = tp // 2, tp % 2
    mate = side * 2 + 1 - core
    across = (1 - side) * 2 + core

    barrier = pltpu.get_barrier_semaphore()

    loads = [
        pltpu.make_async_copy(source, target, load_sem.at[slot])
        for slot, (source, target) in enumerate(
            (
                (filter_hbm, taps),
                (key_hbm, key),
                (value_hbm, value),
                (skip_hbm, skip_ref),
                (first_hbm, first_ref),
                (second_hbm, second_ref),
                (second_back_hbm, second_back_ref),
                (first_back_hbm, first_back_ref),
                (twist_hbm, twist_ref),
                (gate_hbm, gate),
                (weight_hbm, weight),
            )
        )
    ]
    loads[0].start()
    every_peer(
        me,
        lambda other: pl.semaphore_signal(
            barrier, inc=1, device_id={"ctx": other}, device_id_type=MESH
        ),
    )
    for other in (mate, across):
        pl.semaphore_signal(barrier, inc=1, device_id={"tp": other}, device_id_type=MESH)

    for load in loads[1:]:
        load.start()

    def multiply(chunk):
        def step(row, carry):
            product = key[row, chunk].astype(jnp.float32) * value[row, chunk].astype(jnp.float32)
            mixed[row, chunk] = product.astype(jnp.bfloat16)
            return carry

        lax.fori_loop(0, CTX, step, 0, unroll=8)

    def skip():
        for part in range(8):
            spread = jnp.broadcast_to(skip_ref[part : part + 1, :], (128, 128)).T
            for half in range(2):
                rows = mixed[part * 8 : part * 8 + 8, :, :, half * 128 : half * 128 + 128]
                rows = rows.astype(jnp.float32).reshape(128, 128)
                skipped[half, part * 128 : part * 128 + 128, :] = spread * rows

    def sent_in(chunk, which, target):
        source, landing = ((taps, in_taps), (mixed, in_mixed))[which]
        return pltpu.make_async_remote_copy(
            src_ref=source.at[target, chunk],
            dst_ref=landing.at[chunk, me],
            send_sem=in_send_sem.at[chunk, which],
            recv_sem=in_recv_sem.at[chunk, which],
            device_id={"ctx": target},
            device_id_type=MESH,
        )

    def push_in(chunk, which):
        every_peer(me, lambda other: sent_in(chunk, which, other).start())
        source, landing = ((taps, in_taps), (mixed, in_mixed))[which]
        landing[chunk, me] = source[me, chunk]

    def wait_in(chunk, which, receive):
        source, landing = ((taps, in_taps), (mixed, in_mixed))[which]
        whole = landing.at[chunk, pl.ds(0, CTX - 1)]
        copy = pltpu.make_async_remote_copy(
            src_ref=whole,
            dst_ref=whole,
            send_sem=in_send_sem.at[chunk, which],
            recv_sem=in_recv_sem.at[chunk, which],
            device_id={"ctx": (me + 1) % CTX},
            device_id_type=MESH,
        )
        if receive:
            copy.wait_recv()
        else:
            copy.wait_send()

    def spread(chunk, landing, stage):
        def step(row, carry):
            block = landing[chunk, row].astype(jnp.float32)
            stage[row, 0] = block[:, :128]
            stage[row, 1] = block[:, 128:]
            return carry

        lax.fori_loop(0, CTX, step, 0, unroll=8)

    def transform(stage, first_channel):
        cos, sin = twist_ref[0], twist_ref[1]
        flat = stage.reshape(BASE * GROUP, BASE)
        rows = [
            flat[pl.ds(first_channel + one, BASE, stride=GROUP), :].astype(jnp.bfloat16)
            for one in range(SPAN)
        ]
        both = dot(first_ref[...], jnp.concatenate(rows, 1))
        turned = []
        for one in range(SPAN):
            real = both[:BASE, one * BASE : one * BASE + BASE]
            imag = both[BASE:, one * BASE : one * BASE + BASE]
            pieces = [real * cos - imag * sin, real * sin + imag * cos]
            turned.append(jnp.concatenate([piece.astype(jnp.bfloat16) for piece in pieces], 1))
        return dot(jnp.concatenate(turned, 0), second_ref[...])

    def transform_taps(chunk):
        spread(chunk, in_taps, stage_taps)
        for start in range(0, GROUP, SPAN):
            spectra_taps[chunk, start * BASE : (start + SPAN) * BASE, :] = transform(
                stage_taps, start
            )

    def convolve(chunk):
        cos, sin = twist_ref[0], twist_ref[1]
        spread(chunk, in_mixed, stage_mixed)
        flat = stage_out.reshape(BASE * GROUP, BASE)
        for start in range(0, GROUP, SPAN):
            right = transform(stage_mixed, start)
            left = spectra_taps[chunk, start * BASE : (start + SPAN) * BASE, :]
            left_real, left_imag = left[:, :BASE], left[:, BASE:]
            right_real, right_imag = right[:, :BASE], right[:, BASE:]
            real = left_real * right_real - left_imag * right_imag
            imag = left_real * right_imag + left_imag * right_real
            product = jnp.concatenate([real.astype(jnp.bfloat16), imag.astype(jnp.bfloat16)], 1)
            back = dot(product, second_back_ref[...])
            unturned = []
            for one in range(SPAN):
                real = back[one * BASE : one * BASE + BASE, :BASE]
                imag = back[one * BASE : one * BASE + BASE, BASE:]
                pieces = [real * cos + imag * sin, imag * cos - real * sin]
                unturned.append(
                    jnp.concatenate([piece.astype(jnp.bfloat16) for piece in pieces], 0)
                )
            conv = dot(first_back_ref[...], jnp.concatenate(unturned, 1))
            for one in range(SPAN):
                flat[pl.ds(start + one, BASE, stride=GROUP), :] = conv[
                    :, one * BASE : one * BASE + BASE
                ]

        def gather(row, carry):
            for half in range(2):
                back_send[half, chunk, row] = stage_out[row, half].astype(jnp.bfloat16)
            return carry

        lax.fori_loop(0, CTX, gather, 0, unroll=8)
        for half in range(2):
            back_recv[half, me * CHUNKS + chunk] = back_send[half, chunk, me]

    def push_back(half, chunk):
        def send(target):
            pltpu.make_async_remote_copy(
                src_ref=back_send.at[half, chunk, target],
                dst_ref=back_recv.at[half, me * CHUNKS + chunk],
                send_sem=back_send_sem.at[half],
                recv_sem=back_recv_sem.at[half],
                device_id={"ctx": target},
                device_id_type=MESH,
            ).start()

        every_peer(me, send)

    loads[0].wait()
    pl.semaphore_wait(barrier, CTX + 1)
    push_in(0, 0)
    push_in(1, 0)
    loads[1].wait()
    loads[2].wait()
    multiply(0)
    push_in(0, 1)
    multiply(1)
    push_in(1, 1)
    for load in loads[3:9]:
        load.wait()
    skip()
    wait_in(0, 0, True)
    transform_taps(0)
    wait_in(1, 0, True)
    transform_taps(1)
    wait_in(0, 1, True)
    convolve(0)
    push_back(0, 0)
    wait_in(1, 1, True)
    convolve(1)
    push_back(0, 1)
    push_back(1, 0)

    @pl.when(core == 0)
    def _():
        push_back(1, 1)


    def wait_back(half):
        whole = back_recv.at[half, pl.ds(0, (CTX - 1) * CHUNKS)]
        return pltpu.make_async_remote_copy(
            src_ref=whole,
            dst_ref=whole,
            send_sem=back_send_sem.at[half],
            recv_sem=back_recv_sem.at[half],
            device_id={"ctx": (me + 1) % CTX},
            device_id_type=MESH,
        )

    def to_mate(half, slot, piece):
        rows = pl.ds(pl.multiple_of(piece * PIECE, PIECE), PIECE)
        return pltpu.make_async_remote_copy(
            src_ref=core_send.at[half, slot, rows],
            dst_ref=core_recv.at[half, slot, rows],
            send_sem=core_send_sem.at[half, slot, piece],
            recv_sem=core_recv_sem.at[half, slot, piece],
            device_id={"tp": mate},
            device_id_type=MESH,
        )

    def to_across(half, rows):
        return pltpu.make_async_remote_copy(
            src_ref=y_send.at[half, rows],
            dst_ref=other_hbm.at[rows, pl.ds(half * 128, 128)],
            send_sem=y_send_sem.at[half],
            recv_sem=y_recv_sem.at[half],
            device_id={"tp": across},
            device_id_type=MESH,
        )

    def own_out(half):
        return pltpu.make_async_copy(
            own.at[half], own_hbm.at[:, pl.ds(half * 128, 128)], own_sem.at[half]
        )

    loads[9].wait()
    loads[10].wait()
    def gating(half):
        for part in range(8):
            lanes = slice(half * 128, half * 128 + 128)
            block = slice(part * 16, part * 16 + 16)
            conv = back_recv[half, block].astype(jnp.float32).reshape(128, 128)
            gates = gate[block, :, lanes].astype(jnp.float32).reshape(128, 128)
            rows = slice(part * 128, part * 128 + 128)
            gated[half, rows, :] = (gates * (conv + skipped[half, rows, :])).astype(jnp.bfloat16)

    def sums(half, slot):
        owner = (side + 1 - slot) % 2

        def project(piece):
            rows = pl.ds(pl.multiple_of(piece * PIECE, PIECE), PIECE)

            def part(block):
                start = pl.multiple_of(block * 1024 + piece * PIECE, PIECE)
                return dot(weight[pl.ds(start, PIECE), :], gated[half])

            core_send[half, slot, rows, :] = part(owner * 2 + 1 - core).astype(jnp.bfloat16)
            to_mate(half, slot, piece).start()
            keep[half, slot, rows, :] = part(owner * 2 + core)

        def combine(piece):
            rows = pl.ds(pl.multiple_of(piece * PIECE, PIECE), PIECE)
            to_mate(half, slot, piece).wait_recv()
            summed = keep[half, slot, rows, :] + core_recv[half, slot, rows, :].astype(jnp.float32)
            if slot == 0:
                y_send[half, rows, :] = summed.astype(jnp.bfloat16)
                to_across(half, rows).start()
            else:
                own[half, rows, :] = summed.astype(jnp.bfloat16)

        def advance(piece, carry):
            project(piece)

            @pl.when(piece > 0)
            def _():
                combine(piece - 1)

            return carry

        lax.fori_loop(0, PIECES, advance, 0)
        return lambda: combine(PIECES - 1)

    wait_back(0).wait_recv()
    gating(0)

    @pl.when(core == 1)
    def _():
        push_back(1, 1)

    sums(0, 0)()
    wait_back(1).wait_recv()
    gating(1)
    sums(1, 0)()
    sums(0, 1)()
    own_out(0).start()
    sums(1, 1)()
    own_out(1).start()

    for chunk in range(CHUNKS):
        wait_in(chunk, 0, False)
        wait_in(chunk, 1, False)
    for half in range(2):
        wait_back(half).wait_send()
        for slot in range(2):
            for piece in range(PIECES):
                to_mate(half, slot, piece).wait_send()
        own_out(half).wait()
        to_across(half, pl.ds(0, 1024)).wait_send()
        to_across(half, pl.ds(0, 1024)).wait_recv()


def body(gate_branch, key_branch, value_branch, long_filter, skip_gain, out_weight):
    low, full = jnp.bfloat16, jnp.float32
    dma = pltpu.SemaphoreType.DMA
    messages = (CTX, CHUNKS, GROUP, 256)
    anywhere = pl.BlockSpec(memory_space=pl.ANY)
    own, other = pl.pallas_call(
        kernel,
        out_shape=[jax.ShapeDtypeStruct((1024, 256), low)] * 2,
        in_specs=[anywhere] * 11,
        out_specs=[anywhere] * 2,
        scratch_shapes=[
            pltpu.VMEM((128, 8, 256), low),
            pltpu.VMEM(messages, low),
            pltpu.VMEM(messages, low),
            pltpu.VMEM(messages, low),
            pltpu.VMEM((4096, 1024), low),
            pltpu.VMEM(messages, low),
            pltpu.VMEM((2, 1024, 128), full),
            pltpu.VMEM((CHUNKS, CTX, GROUP, 256), low),
            pltpu.VMEM((CHUNKS, CTX, GROUP, 256), low),
            pltpu.VMEM((CTX, 2, GROUP, 128), full),
            pltpu.VMEM((CTX, 2, GROUP, 128), full),
            pltpu.VMEM((CTX, 2, GROUP, 128), full),
            pltpu.VMEM((CHUNKS, GROUP * BASE, 2 * BASE), full),
            pltpu.VMEM((2, CHUNKS, CTX, GROUP, 128), low),
            pltpu.VMEM((2, CTX * CHUNKS, GROUP, 128), low),
            pltpu.VMEM((2, 1024, 128), low),
            pltpu.VMEM((2, 2, 1024, 128), low),
            pltpu.VMEM((2, 2, 1024, 128), low),
            pltpu.VMEM((2, 2, 1024, 128), full),
            pltpu.VMEM((2, 1024, 128), low),
            pltpu.VMEM((2, 1024, 128), low),
            pltpu.VMEM((8, 128), full),
            pltpu.VMEM((2 * BASE, BASE), low),
            pltpu.VMEM((2 * BASE, 2 * BASE), low),
            pltpu.VMEM((2 * BASE, 2 * BASE), low),
            pltpu.VMEM((BASE, 2 * BASE), low),
            pltpu.VMEM((2, BASE, BASE), full),
            dma((11,)),
            dma((CHUNKS, 2)),
            dma((CHUNKS, 2)),
            dma((2,)),
            dma((2,)),
            dma((2, 2, PIECES)),
            dma((2, 2, PIECES)),
            dma((2,)),
            dma((2,)),
            dma((2,)),
        ],
        compiler_params=pltpu.CompilerParams(
            collective_id=0, has_side_effects=True, vmem_limit_bytes=60 * 1024 * 1024
        ),
    )(
        gate_branch.reshape(128, 8, 256),
        key_branch.reshape(messages),
        value_branch.reshape(messages),
        long_filter.reshape(messages),
        skip_gain.reshape(8, 128),
        out_weight,
        *tables(),
    )
    return (own.astype(full) + other.astype(full)).astype(low)


def solution(mesh):
    placed = (
        P("tp", "ctx"),
        P("tp", "ctx"),
        P("tp", "ctx"),
        P("tp", "ctx"),
        P("tp"),
        P(None, "tp"),
    )
    return jax.shard_map(
        body, mesh=mesh, in_specs=placed, out_specs=P("tp", "ctx"), check_vma=False
    )
```

```python
import functools

import jax
import jax.numpy as jnp
import numpy as np
from jax import lax
from jax.experimental import pallas as pl
from jax.experimental.pallas import tpu as pltpu
from jax.sharding import PartitionSpec as P

MESH = pl.DeviceIdType.MESH
CTX = 64
TP = 4
BASE = 128
CHUNKS = 2
GROUP = 8
SPAN = 8
PIECE = 256
PIECES = 1024 // PIECE


def tables():
    index = np.arange(BASE)
    first = np.exp(2j * np.pi * np.outer(index + 0.25, index) / BASE)
    twist = np.exp(2j * np.pi * np.outer(index + 0.25, index) / BASE**2)
    second = np.exp(2j * np.pi * np.outer(index, index) / BASE)
    back = first.T / BASE**2
    low = lambda table: jnp.asarray(table, jnp.bfloat16)
    return (
        low(np.concatenate([first.real, first.imag], 0)),
        low(np.block([[second.real, second.imag], [-second.imag, second.real]])),
        low(np.block([[second.real, -second.imag], [second.imag, second.real]])),
        low(np.concatenate([back.real, back.imag], 1)),
        jnp.asarray(np.stack([twist.real, twist.imag]), jnp.float32),
    )


def every_peer(me, act):
    high, z, x = me // 32 * 32, (me // 4) % 8, me % 4
    near = [(x + step) % 4 for step in range(4)]
    far = [(z + step) % 8 * 4 for step in range(8)]
    halves = (high, 32 - high)
    for dz, dy, dx in ORDER:
        act(halves[dy] + far[dz] + near[dx])


def every_peer_root_first(me, act):
    high, z, x = me // 32, (me // 4) % 8, me % 4
    near = [(x + step) % 4 for step in range(4)]
    far = [(z + step) % 8 for step in range(8)]
    halves = (high, 1 - high)
    for first_z in (0, 7, 1):
        for first_x in (0, 3, 1):
            target = first_z * 4 + first_x

            @pl.when(target != me)
            def _(target=target):
                act(target)

    z_first = [(place + 1) % 8 <= 2 for place in far]
    x_first = [(place + 1) % 4 <= 2 for place in near]
    y_first = [place == 0 for place in halves]
    for dz, dy, dx in ORDER:
        first = jnp.logical_and(jnp.logical_and(z_first[dz], x_first[dx]), y_first[dy])

        @pl.when(jnp.logical_not(first))
        def _(dz=dz, dy=dy, dx=dx):
            act(halves[dy] * 32 + far[dz] * 4 + near[dx])


ORDER = [(4, 1, 2), (3, 1, 2), (4, 1, 1), (4, 1, 3), (5, 1, 2), (2, 1, 2), (3, 1, 1), (3, 1, 3), (4, 0, 2), (4, 1, 0), (5, 1, 1), (5, 1, 3), (6, 1, 2), (1, 1, 2), (2, 1, 1), (2, 1, 3), (3, 0, 2), (3, 1, 0), (4, 0, 1), (4, 0, 3), (5, 0, 2), (5, 1, 0), (6, 1, 1), (6, 1, 3), (7, 1, 2), (0, 1, 2), (1, 1, 1), (1, 1, 3), (2, 0, 2), (2, 1, 0), (3, 0, 1), (3, 0, 3), (4, 0, 0), (5, 0, 1), (5, 0, 3), (6, 0, 2), (6, 1, 0), (7, 1, 1), (7, 1, 3), (0, 1, 1), (0, 1, 3), (1, 0, 2), (1, 1, 0), (2, 0, 1), (2, 0, 3), (3, 0, 0), (5, 0, 0), (6, 0, 1), (6, 0, 3), (7, 0, 2), (7, 1, 0), (0, 0, 2), (0, 1, 0), (1, 0, 1), (1, 0, 3), (2, 0, 0), (6, 0, 0), (7, 0, 1), (7, 0, 3), (0, 0, 1), (0, 0, 3), (1, 0, 0), (7, 0, 0)]


def dot(left, right):
    return jnp.dot(left, right, preferred_element_type=jnp.float32)


def kernel(
    gate_hbm,
    key_hbm,
    value_hbm,
    filter_hbm,
    skip_hbm,
    weight_hbm,
    first_hbm,
    second_hbm,
    second_back_hbm,
    first_back_hbm,
    twist_hbm,
    own_hbm,
    other_hbm,
    gate,
    key,
    value,
    taps,
    weight,
    mixed,
    skipped,
    in_mixed,
    in_taps,
    stage_mixed,
    stage_taps,
    stage_out,
    spectra_taps,
    back_send,
    back_recv,
    gated,
    core_send,
    core_recv,
    keep,
    y_send,
    own,
    skip_ref,
    first_ref,
    second_ref,
    second_back_ref,
    first_back_ref,
    twist_ref,
    load_sem,
    taps_send_sem,
    taps_recv_sem,
    in_send_sem,
    in_recv_sem,
    back_send_sem,
    back_recv_sem,
    core_send_sem,
    core_recv_sem,
    y_send_sem,
    y_recv_sem,
    own_sem,
):
    me, tp = lax.axis_index("ctx"), lax.axis_index("tp")
    side, core = tp // 2, tp % 2
    mate = side * 2 + 1 - core
    across = (1 - side) * 2 + core

    barrier = pltpu.get_barrier_semaphore()

    loads = [
        pltpu.make_async_copy(source, target, load_sem.at[slot])
        for slot, (source, target) in enumerate(
            (
                (filter_hbm, taps),
                (key_hbm, key),
                (value_hbm, value),
                (skip_hbm, skip_ref),
                (first_hbm, first_ref),
                (second_hbm, second_ref),
                (second_back_hbm, second_back_ref),
                (first_back_hbm, first_back_ref),
                (twist_hbm, twist_ref),
                (gate_hbm, gate),
                (weight_hbm, weight),
            )
        )
    ]
    loads[0].start()
    every_peer(
        me,
        lambda other: pl.semaphore_signal(
            barrier, inc=1, device_id={"ctx": other}, device_id_type=MESH
        ),
    )
    for other in (mate, across):
        pl.semaphore_signal(barrier, inc=1, device_id={"tp": other}, device_id_type=MESH)

    for load in loads[1:]:
        load.start()

    def multiply(chunk):
        def step(row, carry):
            product = key[row, chunk].astype(jnp.float32) * value[row, chunk].astype(jnp.float32)
            mixed[row, chunk] = product.astype(jnp.bfloat16)
            return carry

        lax.fori_loop(0, CTX, step, 0, unroll=8)

    def skip():
        for part in range(8):
            spread = jnp.broadcast_to(skip_ref[part : part + 1, :], (128, 128)).T
            for half in range(2):
                rows = mixed[part * 8 : part * 8 + 8, :, :, half * 128 : half * 128 + 128]
                rows = rows.astype(jnp.float32).reshape(128, 128)
                skipped[half, part * 128 : part * 128 + 128, :] = spread * rows

    def sent_taps(target, landing):
        return pltpu.make_async_remote_copy(
            src_ref=taps.at[target],
            dst_ref=in_taps.at[landing],
            send_sem=taps_send_sem,
            recv_sem=taps_recv_sem,
            device_id={"ctx": target},
            device_id_type=MESH,
        )

    def sent_mixed(chunk, target):
        return pltpu.make_async_remote_copy(
            src_ref=mixed.at[target, chunk],
            dst_ref=in_mixed.at[chunk, me],
            send_sem=in_send_sem.at[chunk],
            recv_sem=in_recv_sem.at[chunk],
            device_id={"ctx": target},
            device_id_type=MESH,
        )

    def push_taps():
        every_peer(me, lambda other: sent_taps(other, me).start())
        in_taps[me] = taps[me]

    def push_mixed(chunk):
        every_peer(me, lambda other: sent_mixed(chunk, other).start())
        in_mixed[chunk, me] = mixed[me, chunk]

    def all_taps():
        whole = in_taps.at[pl.ds(0, CTX - 1)]
        return pltpu.make_async_remote_copy(
            src_ref=whole,
            dst_ref=whole,
            send_sem=taps_send_sem,
            recv_sem=taps_recv_sem,
            device_id={"ctx": (me + 1) % CTX},
            device_id_type=MESH,
        )

    def all_mixed(chunk):
        whole = in_mixed.at[chunk, pl.ds(0, CTX - 1)]
        return pltpu.make_async_remote_copy(
            src_ref=whole,
            dst_ref=whole,
            send_sem=in_send_sem.at[chunk],
            recv_sem=in_recv_sem.at[chunk],
            device_id={"ctx": (me + 1) % CTX},
            device_id_type=MESH,
        )

    def spread(take, stage):
        def step(row, carry):
            block = take(row).astype(jnp.float32)
            stage[row, 0] = block[:, :128]
            stage[row, 1] = block[:, 128:]
            return carry

        lax.fori_loop(0, CTX, step, 0, unroll=8)

    def transform(stage, first_channel):
        cos, sin = twist_ref[0], twist_ref[1]
        flat = stage.reshape(BASE * GROUP, BASE)
        rows = [
            flat[pl.ds(first_channel + one, BASE, stride=GROUP), :].astype(jnp.bfloat16)
            for one in range(SPAN)
        ]
        both = dot(first_ref[...], jnp.concatenate(rows, 1))
        turned = []
        for one in range(SPAN):
            real = both[:BASE, one * BASE : one * BASE + BASE]
            imag = both[BASE:, one * BASE : one * BASE + BASE]
            pieces = [real * cos - imag * sin, real * sin + imag * cos]
            turned.append(jnp.concatenate([piece.astype(jnp.bfloat16) for piece in pieces], 1))
        return dot(jnp.concatenate(turned, 0), second_ref[...])

    def transform_taps(chunk):
        spread(lambda row: in_taps[row, chunk], stage_taps)
        for start in range(0, GROUP, SPAN):
            spectra_taps[chunk, start * BASE : (start + SPAN) * BASE, :] = transform(
                stage_taps, start
            )

    def convolve(chunk):
        cos, sin = twist_ref[0], twist_ref[1]
        spread(lambda row: in_mixed[chunk, row], stage_mixed)
        flat = stage_out.reshape(BASE * GROUP, BASE)
        for start in range(0, GROUP, SPAN):
            right = transform(stage_mixed, start)
            left = spectra_taps[chunk, start * BASE : (start + SPAN) * BASE, :]
            left_real, left_imag = left[:, :BASE], left[:, BASE:]
            right_real, right_imag = right[:, :BASE], right[:, BASE:]
            real = left_real * right_real - left_imag * right_imag
            imag = left_real * right_imag + left_imag * right_real
            product = jnp.concatenate([real.astype(jnp.bfloat16), imag.astype(jnp.bfloat16)], 1)
            back = dot(product, second_back_ref[...])
            unturned = []
            for one in range(SPAN):
                real = back[one * BASE : one * BASE + BASE, :BASE]
                imag = back[one * BASE : one * BASE + BASE, BASE:]
                pieces = [real * cos + imag * sin, imag * cos - real * sin]
                unturned.append(
                    jnp.concatenate([piece.astype(jnp.bfloat16) for piece in pieces], 0)
                )
            conv = dot(first_back_ref[...], jnp.concatenate(unturned, 1))
            for one in range(SPAN):
                flat[pl.ds(start + one, BASE, stride=GROUP), :] = conv[
                    :, one * BASE : one * BASE + BASE
                ]

        def gather(row, carry):
            for half in range(2):
                back_send[half, row, chunk] = stage_out[row, half].astype(jnp.bfloat16)
            return carry

        lax.fori_loop(0, CTX, gather, 0, unroll=8)
        for half in range(2):
            back_recv[half, me, chunk] = back_send[half, me, chunk]

    def push_back(half, chunks):
        def send(target):
            pltpu.make_async_remote_copy(
                src_ref=back_send.at[half, target, chunks],
                dst_ref=back_recv.at[half, me, chunks],
                send_sem=back_send_sem.at[half],
                recv_sem=back_recv_sem.at[half],
                device_id={"ctx": target},
                device_id_type=MESH,
            ).start()

        every_peer_root_first(me, send)

    first_chunk, last_chunk, both_chunks = pl.ds(0, 1), pl.ds(1, 1), pl.ds(0, 2)
    loads[0].wait()
    pl.semaphore_wait(barrier, CTX + 1)
    push_taps()
    loads[1].wait()
    loads[2].wait()
    multiply(0)
    push_mixed(0)
    multiply(1)
    push_mixed(1)
    for load in loads[3:9]:
        load.wait()
    skip()
    all_taps().wait_recv()
    transform_taps(0)
    transform_taps(1)
    all_mixed(0).wait_recv()
    convolve(0)
    push_back(0, first_chunk)
    all_mixed(1).wait_recv()
    convolve(1)
    push_back(0, last_chunk)

    @pl.when(core == 0)
    def _():
        push_back(1, both_chunks)

    @pl.when(core == 1)
    def _():
        push_back(1, first_chunk)


    def wait_back(half):
        whole = back_recv.at[half, pl.ds(0, CTX - 1)]
        return pltpu.make_async_remote_copy(
            src_ref=whole,
            dst_ref=whole,
            send_sem=back_send_sem.at[half],
            recv_sem=back_recv_sem.at[half],
            device_id={"ctx": (me + 1) % CTX},
            device_id_type=MESH,
        )

    def to_mate(half, slot, piece):
        rows = pl.ds(pl.multiple_of(piece * PIECE, PIECE), PIECE)
        return pltpu.make_async_remote_copy(
            src_ref=core_send.at[half, slot, rows],
            dst_ref=core_recv.at[half, slot, rows],
            send_sem=core_send_sem.at[half, slot, piece],
            recv_sem=core_recv_sem.at[half, slot, piece],
            device_id={"tp": mate},
            device_id_type=MESH,
        )

    def to_across(half, rows):
        return pltpu.make_async_remote_copy(
            src_ref=y_send.at[half, rows],
            dst_ref=other_hbm.at[rows, pl.ds(half * 128, 128)],
            send_sem=y_send_sem.at[half],
            recv_sem=y_recv_sem.at[half],
            device_id={"tp": across},
            device_id_type=MESH,
        )

    def own_out(half):
        return pltpu.make_async_copy(
            own.at[half], own_hbm.at[:, pl.ds(half * 128, 128)], own_sem.at[half]
        )

    loads[9].wait()
    loads[10].wait()
    def gating(half):
        for part in range(8):
            lanes = slice(half * 128, half * 128 + 128)
            block = slice(part * 16, part * 16 + 16)
            conv = back_recv[half, part * 8 : part * 8 + 8].astype(jnp.float32).reshape(128, 128)
            gates = gate[block, :, lanes].astype(jnp.float32).reshape(128, 128)
            rows = slice(part * 128, part * 128 + 128)
            gated[half, rows, :] = (gates * (conv + skipped[half, rows, :])).astype(jnp.bfloat16)

    def sums(half, slot):
        owner = (side + 1 - slot) % 2

        def project(piece):
            rows = pl.ds(pl.multiple_of(piece * PIECE, PIECE), PIECE)

            def part(block):
                start = pl.multiple_of(block * 1024 + piece * PIECE, PIECE)
                return dot(weight[pl.ds(start, PIECE), :], gated[half])

            core_send[half, slot, rows, :] = part(owner * 2 + 1 - core).astype(jnp.bfloat16)
            to_mate(half, slot, piece).start()
            keep[half, slot, rows, :] = part(owner * 2 + core)

        def combine(piece):
            rows = pl.ds(pl.multiple_of(piece * PIECE, PIECE), PIECE)
            to_mate(half, slot, piece).wait_recv()
            summed = keep[half, slot, rows, :] + core_recv[half, slot, rows, :].astype(jnp.float32)
            if slot == 0:
                y_send[half, rows, :] = summed.astype(jnp.bfloat16)
                to_across(half, rows).start()
            else:
                own[half, rows, :] = summed.astype(jnp.bfloat16)

        def advance(piece, carry):
            project(piece)

            @pl.when(piece > 0)
            def _():
                combine(piece - 1)

            return carry

        lax.fori_loop(0, PIECES, advance, 0)
        return lambda: combine(PIECES - 1)

    wait_back(0).wait_recv()

    @pl.when(core == 1)
    def _():
        push_back(1, last_chunk)

    gating(0)
    sums(0, 0)()
    wait_back(1).wait_recv()
    gating(1)
    sums(1, 0)()
    sums(0, 1)()
    own_out(0).start()
    sums(1, 1)()
    own_out(1).start()

    all_taps().wait_send()
    for chunk in range(CHUNKS):
        all_mixed(chunk).wait_send()
    for half in range(2):
        wait_back(half).wait_send()
        for slot in range(2):
            for piece in range(PIECES):
                to_mate(half, slot, piece).wait_send()
        own_out(half).wait()
        to_across(half, pl.ds(0, 1024)).wait_send()
        to_across(half, pl.ds(0, 1024)).wait_recv()


def body(gate_branch, key_branch, value_branch, long_filter, skip_gain, out_weight):
    low, full = jnp.bfloat16, jnp.float32
    dma = pltpu.SemaphoreType.DMA
    messages = (CTX, CHUNKS, GROUP, 256)
    anywhere = pl.BlockSpec(memory_space=pl.ANY)
    own, other = pl.pallas_call(
        kernel,
        out_shape=[jax.ShapeDtypeStruct((1024, 256), low)] * 2,
        in_specs=[anywhere] * 11,
        out_specs=[anywhere] * 2,
        scratch_shapes=[
            pltpu.VMEM((128, 8, 256), low),
            pltpu.VMEM(messages, low),
            pltpu.VMEM(messages, low),
            pltpu.VMEM(messages, low),
            pltpu.VMEM((4096, 1024), low),
            pltpu.VMEM(messages, low),
            pltpu.VMEM((2, 1024, 128), full),
            pltpu.VMEM((CHUNKS, CTX, GROUP, 256), low),
            pltpu.VMEM(messages, low),
            pltpu.VMEM((CTX, 2, GROUP, 128), full),
            pltpu.VMEM((CTX, 2, GROUP, 128), full),
            pltpu.VMEM((CTX, 2, GROUP, 128), full),
            pltpu.VMEM((CHUNKS, GROUP * BASE, 2 * BASE), full),
            pltpu.VMEM((2, CTX, CHUNKS, GROUP, 128), low),
            pltpu.VMEM((2, CTX, CHUNKS, GROUP, 128), low),
            pltpu.VMEM((2, 1024, 128), low),
            pltpu.VMEM((2, 2, 1024, 128), low),
            pltpu.VMEM((2, 2, 1024, 128), low),
            pltpu.VMEM((2, 2, 1024, 128), full),
            pltpu.VMEM((2, 1024, 128), low),
            pltpu.VMEM((2, 1024, 128), low),
            pltpu.VMEM((8, 128), full),
            pltpu.VMEM((2 * BASE, BASE), low),
            pltpu.VMEM((2 * BASE, 2 * BASE), low),
            pltpu.VMEM((2 * BASE, 2 * BASE), low),
            pltpu.VMEM((BASE, 2 * BASE), low),
            pltpu.VMEM((2, BASE, BASE), full),
            dma((11,)),
            dma(()),
            dma(()),
            dma((CHUNKS,)),
            dma((CHUNKS,)),
            dma((2,)),
            dma((2,)),
            dma((2, 2, PIECES)),
            dma((2, 2, PIECES)),
            dma((2,)),
            dma((2,)),
            dma((2,)),
        ],
        compiler_params=pltpu.CompilerParams(
            collective_id=0, has_side_effects=True, vmem_limit_bytes=60 * 1024 * 1024
        ),
    )(
        gate_branch.reshape(128, 8, 256),
        key_branch.reshape(messages),
        value_branch.reshape(messages),
        long_filter.reshape(messages),
        skip_gain.reshape(8, 128),
        out_weight,
        *tables(),
    )
    return (own.astype(full) + other.astype(full)).astype(low)


def solution(mesh):
    placed = (
        P("tp", "ctx"),
        P("tp", "ctx"),
        P("tp", "ctx"),
        P("tp", "ctx"),
        P("tp"),
        P(None, "tp"),
    )
    return jax.shard_map(
        body, mesh=mesh, in_specs=placed, out_specs=P("tp", "ctx"), check_vma=False
    )
```
